256 devices in a mesh: groups: 2 (over z), roll: 16 (over y, core), rows: 8 (over x).
Axes of the slice: x: 8, y: 8, z: 2, core: 2. Of those that a mesh axis runs over, the one named last changes fastest.
The devices are a block of a 8x8x16 slice.
Arguments:
- latent_slabs: bfloat16 [64, 3, 64, 8, 16], P(('groups', 'roll'), None, 'rows'), parts along dimension 0, may hold values from -18 to 18, as said below
- prior_latents: bfloat16 [64, 2, 64, 8, 16], P(('groups', 'roll'), None, 'rows'), parts along dimension 0, may hold values from -6 to 6
- prior_features: bfloat16 [64, 2, 64, 8, 512], P(('groups', 'roll'), None, 'rows'), parts along dimension 0, may hold values from -6 to 6
- lengths: int32 [64], P(('groups', 'roll')), parts along dimension 0, may hold values from 1 to 3
- starts: int32 [64], P(('groups', 'roll')), parts along dimension 0, may hold values from 0 to 6, as said below
- move_plan: int32 [64], P(('groups', 'roll')), parts along dimension 0, may hold values from -1 to 15, as said below
- entry_weight: bfloat16 [432, 512], replicated, may hold values from -0.3125 to 0.3125
- block_weight: bfloat16 [13824, 512], P(None, ('roll', 'rows')), may hold values from -0.0546875 to 0.0546875
- norm_gain: float32 [512], replicated, may hold values from 0.25 to 1.75
- norm_shift: float32 [512], replicated, may hold values from -1.2 to 1.2
Outputs:
- decoded: bfloat16 [64, 3, 64, 8, 512], P(('groups', 'roll'), None, 'rows'), parts along dimension 0
The draws below stay inside these ranges and needn't reach their ends.
There are 2 independent parts, one for each index of `groups`. The reference program is written for one: setup_inputs(seed, part) draws one part's arguments, and reference() takes and returns one part's arrays. A program takes and returns all parts, laid end to end along the dimension named above; an argument that names none is the same for every part. Nothing has to cross between parts.
Inputs may be any that keep to these rules, and one draw needn't show every extreme that they name: `latent_slabs`: normal or uniform values times a scale that varies over the rows. `starts`: multiples of 3. `move_plan`: A value d * 1 + c names compute slot c of roll index d. Every compute slot of the part is named by exactly one slab, and the slabs held by one roll index name at most 1 slots of any one roll index.
All inputs are finite; a program needn't handle non-finite values.
Results may differ from the reference program's by a relative error of at most 0.0023.
Values may be sent and summed in bfloat16 or wider, within the bound.
No kernel may reach another device: no remote copies, remote signals or barrier semaphores. Data moves between devices by JAX's collectives and lax.ppermute only.
A program may use at most 128 MiB of HBM per device.

```python
import jax
import jax.numpy as jnp
from jax import lax

LAT = 16
FEAT = 512
GROUPS = 32
FRAMES = 3
COLS = 8
ROLL_DEV = 2
CAP = 1
SLABS = 32
HEIGHT = 64
N_ROLL = 16


def draw_latent_slabs(key, part):
    shape_full = (SLABS, FRAMES, HEIGHT, COLS, LAT)
    height_pos = jnp.arange(HEIGHT, dtype=jnp.float32) / max(HEIGHT - 1, 1)
    values = jnp.clip(jax.random.normal(jax.random.fold_in(key, 3), shape_full, jnp.float32), -6.0, 6.0)
    rising = jnp.exp(jnp.log(3.0) * height_pos)
    return (values * rising[None, None, :, None, None]).astype(jnp.bfloat16)


def draw_starts(key, part):
    return (FRAMES * jax.random.randint(jax.random.fold_in(key, 5), (SLABS,), 0, 3)).astype(jnp.int32)


def draw_move_plan(key, part):
    owners = jnp.arange(SLABS) // ROLL_DEV
    leaning = jax.random.randint(jax.random.fold_in(key, 7), (N_ROLL,), 0, 4)
    favored = jax.random.randint(jax.random.fold_in(key, 8), (), 0, N_ROLL)
    leaning = jnp.where(jnp.arange(N_ROLL) == favored, 16, leaning)
    jitter = jax.random.randint(jax.random.fold_in(key, 9), (SLABS,), 0, 64)
    scores = (jitter + 48 * leaning[owners]) * SLABS + jnp.arange(SLABS)
    ranking = jnp.argsort(-scores)
    chosen = jnp.zeros((SLABS,), jnp.int32).at[ranking[:CAP * N_ROLL]].set(1)
    counter = jnp.cumsum(chosen) - 1
    return jnp.where(chosen > 0, counter % N_ROLL * CAP + counter // N_ROLL, -1).astype(jnp.int32)


def touch_ends(entries, stream_key, least, largest):
    longest = entries.shape.index(max(entries.shape))
    spots = []
    for shift in (0, 1):
        where = [jax.random.randint(jax.random.fold_in(stream_key, axis), (), 0, length) for axis, length in enumerate(entries.shape)]
        where[longest] = (where[longest] + shift) % entries.shape[longest]
        spots.append(tuple(where))
    return entries.at[spots[0]].set(least).at[spots[1]].set(largest)


def steps_of(rng, dims, cuts, least, top_value):
    level, own = 1.0, jax.random.fold_in(rng, 6)
    for position, blocks in cuts:
        steps = jnp.exp(jax.random.uniform(jax.random.fold_in(own, position), (blocks,), jnp.float32, least / len(cuts), top_value / len(cuts)))
        level = level * jnp.repeat(steps, dims[position] // blocks).reshape([-1 if axis == position else 1 for axis in range(len(dims))])
    return level


def normal_values(stream_key, dims, spread, bound, pieces=(), held_as=jnp.bfloat16):
    loudness = steps_of(stream_key, dims, pieces, -0.22, 0.18) if pieces else 1.0
    result = jax.random.normal(stream_key, dims, jnp.float32) * spread * loudness
    return jnp.minimum(jnp.maximum(result, -bound), bound).astype(held_as)


def setup_inputs(seed: int = 0, part: int = 0) -> dict:
    key_of = jax.random.split(jax.random.key(seed), 11)
    part_splits = jax.random.split(jax.random.fold_in(key_of[10], part), 11)
    latent_slabs = draw_latent_slabs(jax.random.fold_in(jax.random.fold_in(key_of[10], part), 71), part)
    prior_latents = normal_values(part_splits[1], (SLABS, 2, HEIGHT, COLS, LAT), 1.0, 6.0, ((0, 16), (2, 8)))
    prior_features = normal_values(part_splits[2], (SLABS, 2, HEIGHT, COLS, FEAT), 1.0, 6.0, ((0, 16), (2, 8)))
    lengths = touch_ends(jax.random.randint(part_splits[3], (SLABS,), 1, FRAMES + 1), jax.random.fold_in(part_splits[3], 1), 1, FRAMES).astype(jnp.int32)
    starts = draw_starts(jax.random.fold_in(jax.random.fold_in(key_of[10], part), 71), part)
    move_plan = draw_move_plan(jax.random.fold_in(jax.random.fold_in(key_of[10], part), 71), part)
    entry_weight = normal_values(key_of[6], (27 * LAT, FEAT), (27 * LAT) ** -0.5, 0.3125)
    block_weight = normal_values(key_of[7], (27 * FEAT, FEAT), (27 * FEAT) ** -0.5, 0.0546875, ((1, 128),))
    norm_gain = jnp.clip(1.0 + 0.15 * jax.random.normal(key_of[8], (FEAT,), jnp.float32), 0.25, 1.75)
    norm_shift = normal_values(key_of[9], (FEAT,), 0.3, 1.2, (), jnp.float32)
    return {"latent_slabs": latent_slabs, "prior_latents": prior_latents, "prior_features": prior_features, "lengths": lengths, "starts": starts, "move_plan": move_plan, "entry_weight": entry_weight, "block_weight": block_weight, "norm_gain": norm_gain, "norm_shift": norm_shift}


EPSILON = 1e-06

def convolve(extended, weights):
    frames = extended.shape[0] - 2
    height = extended.shape[1] - 2
    widths = extended.shape[2] - 2
    channels = extended.shape[3]
    accumulated = jnp.zeros((frames * height * widths, weights.shape[1]), jnp.float32)
    for tap_index in range(27):
        step_t = tap_index // 9
        step_h = tap_index // 3 % 3
        step_w = tap_index % 3
        window = extended[step_t:step_t + frames, step_h:step_h + height, step_w:step_w + widths, :]
        accumulated = accumulated + jnp.dot(window.reshape(-1, channels), weights[tap_index * channels:(tap_index + 1) * channels], preferred_element_type=jnp.float32, precision=lax.Precision.HIGHEST)
    return accumulated.reshape(frames, height, widths, weights.shape[1])

def reference(latent_slabs, prior_latents, prior_features, lengths, starts, move_plan, entry_weight, block_weight, norm_gain, norm_shift):
    entry_full = entry_weight.astype(jnp.float32)
    block_full = block_weight.astype(jnp.float32)
    gain_vector = norm_gain.astype(jnp.float32)
    shift_vector = norm_shift.astype(jnp.float32)

    def decode_slab(element):
        latent, prior_lat, prior_feat, length, first_frame, target = element
        cached = first_frame > 0
        prior_lat = jnp.where(cached, prior_lat, jnp.zeros_like(prior_lat))
        prior_feat = jnp.where(cached, prior_feat, jnp.zeros_like(prior_feat))
        stacked = jnp.concatenate([prior_lat, latent], axis=0).astype(jnp.float32)
        hidden = convolve(jnp.pad(stacked, ((0, 0), (1, 1), (1, 1), (0, 0))), entry_full)
        frames, height, widths, features = hidden.shape
        grouped = hidden.reshape(frames, height, widths, GROUPS, features // GROUPS)
        group_mean = lax.optimization_barrier(jnp.mean(grouped, axis=(1, 2, 4)))
        square_mean = lax.optimization_barrier(jnp.mean(grouped * grouped, axis=(1, 2, 4)))
        scaled = lax.rsqrt(square_mean - group_mean * group_mean + EPSILON)
        normed = ((grouped - group_mean[:, None, None, :, None]) * scaled[:, None, None, :, None]).reshape(hidden.shape)
        normed = normed * gain_vector + shift_vector
        active = jax.nn.silu(normed).astype(jnp.bfloat16)
        feature_stack = jnp.concatenate([prior_feat, active], axis=0).astype(jnp.float32)
        mixed_sum = convolve(jnp.pad(feature_stack, ((0, 0), (1, 1), (1, 1), (0, 0))), block_full)
        alive_frames = (jnp.arange(frames) < length) & (target >= 0)
        return jnp.where(alive_frames[:, None, None, None], hidden + mixed_sum, 0.0).astype(jnp.bfloat16)
    return lax.map(decode_slab, (latent_slabs, prior_latents, prior_features, lengths, starts, move_plan))
```

```python
import jax
import jax.numpy as jnp
from jax import lax
from jax.experimental import pallas as pl
from jax.experimental.pallas import tpu as pltpu
from jax.sharding import PartitionSpec as P

GROUPS = 32
EPSILON = 1e-06
MIB = 1 << 20


def nt_dot(a, b):
    return lax.dot_general(a, b, (((1,), (1,)), ((), ())), preferred_element_type=jnp.float32)


def entry_kernel(count, me_ref, *refs):
    lat_refs = refs[:count]
    wk_ref, wown_ref, gain_ref, shift_ref, act_ref, hid_ref, win, lhs, hid, sums = refs[count:]
    slots, total, height, lanes = lat_refs[0].shape
    frames = total - 2
    cells = count * height * 8
    win[:, :, 0:8, :] = jnp.zeros((slots, total, 8, lanes), jnp.float32)
    win[:, :, cells + 8 : cells + 16, :] = jnp.zeros((slots, total, 8, lanes), jnp.float32)
    rows = slots * total * height
    lane = lax.broadcasted_iota(jnp.int32, (rows * 8, lanes), 1)
    col = lax.broadcasted_iota(jnp.int32, (rows * 8, lanes), 0) % 8
    first = jnp.where(col == 7, 16, 0)
    last = jnp.where(col == 0, 32, 48)
    keep = (lane >= first) & (lane < last)
    for d in range(count):
        xp = lax.rem(me_ref[0] + (count - d), count)
        v = lat_refs[d][...].astype(jnp.float32).reshape(rows, 1, lanes)
        v = jnp.broadcast_to(v, (rows, 8, lanes)).reshape(rows * 8, lanes)
        v = pltpu.roll(v, 0, 1, stride=16, stride_axis=0)
        v = jnp.where(keep, v, 0.0)
        v = v + pltpu.roll(v, 64, 1)
        start = pl.multiple_of(8 + xp * (height * 8), 8)
        win[:, :, pl.ds(start, height * 8), :] = v.reshape(slots, total, height * 8, lanes)
    low = lax.broadcasted_iota(jnp.int32, (cells, lanes), 1) < 64
    for s in range(slots):
        for f in range(frames):
            blk = s * frames + f
            for p in range(5):
                t, h = divmod(2 * p, 3)
                a = win[s, f + t, h * 8 : h * 8 + cells, :]
                if p < 4:
                    t, h = divmod(2 * p + 1, 3)
                    a = jnp.where(low, a, win[s, f + t, h * 8 : h * 8 + cells, :])
                lhs[:, p * lanes : (p + 1) * lanes] = a.astype(jnp.bfloat16)
            x = lhs[...]
            y = jnp.dot(x, wk_ref[...], preferred_element_type=jnp.float32)
            hid[blk * cells : (blk + 1) * cells, :] = y
            sums[blk : blk + 1, :] = jnp.sum(y, axis=0, keepdims=True)
            sums[8 + blk : 9 + blk, :] = jnp.sum(y * y, axis=0, keepdims=True)
            hid_ref[f, :, s * 64 : s * 64 + 64] = jnp.dot(
                x, wown_ref[...], preferred_element_type=jnp.float32
            )
    features = gain_ref.shape[1]
    size = features // GROUPS
    gi = lax.broadcasted_iota(jnp.int32, (features, features), 0) // size
    gj = lax.broadcasted_iota(jnp.int32, (features, features), 1) // size
    same = jnp.where(gi == gj, 1.0, 0.0).astype(jnp.float32)
    means = jnp.dot(
        sums[...], same, precision=lax.Precision.HIGHEST, preferred_element_type=jnp.float32
    ) / (cells * size)
    mean = means[0:8]
    spread = means[8:16] - mean * mean
    scale = lax.rsqrt(spread + EPSILON) * gain_ref[...]
    offset = shift_ref[...] - mean * scale
    for s in range(slots):
        for f in range(frames):
            blk = s * frames + f
            z = hid[blk * cells : (blk + 1) * cells, :] * scale[blk : blk + 1] + offset[blk : blk + 1]
            act = (0.5 * z) * (1.0 + jnp.tanh(0.5 * z))
            act_ref[s, f] = act.astype(jnp.bfloat16)


def taps_of(w_ref, t, h):
    k = w_ref.shape[1] // 27
    base = (t * 3 + h) * 3
    return jnp.concatenate([w_ref[:, (base + w) * k : (base + w + 1) * k] for w in range(3)], axis=0)


def new_frames_kernel(act_ref, w_ref, acc_ref):
    slots, frames, cells, _ = act_ref.shape
    acc_ref[...] = jnp.zeros(acc_ref.shape, jnp.float32)
    for h in range(3):
        for t in range(3):
            taps = taps_of(w_ref, t, h)
            for s in range(slots):
                for f in range(frames):
                    if 0 <= f + t - 2 < frames:
                        y = nt_dot(act_ref[s, f + t - 2], taps)
                        at = (2 - h) * 8
                        acc_ref[s, f, at : at + cells, :] += y


def old_frames_kernel(count, me_ref, starts_ref, lengths_ref, plan_ref, *refs):
    feat_refs = refs[:count]
    w_ref, acc_ref, hid_ref, out_ref, feats, acc = refs[count:]
    slots, frames, padded_cells, _ = acc_ref.shape
    cells = padded_cells - 16
    part = cells // count
    for d in range(count):
        xp = lax.rem(me_ref[0] + (count - d), count)
        start = pl.multiple_of(xp * part, part)
        for s in range(slots):
            v = feat_refs[d][s]
            feats[s, :, pl.ds(start, part), :] = jnp.where(starts_ref[s] > 0, v, jnp.zeros_like(v))
    acc[...] = acc_ref[...]
    for h in range(3):
        at = (2 - h) * 8
        for t in range(2):
            taps = taps_of(w_ref, t, h)
            for s in range(slots):
                for f in range(frames):
                    if f + t < 2:
                        acc[s, f, at : at + cells, :] += nt_dot(feats[s, f + t], taps)
    col = lax.broadcasted_iota(jnp.int32, (cells // 8, 8, 64), 1)
    for f in range(frames):
        parts = []
        for s in range(slots):
            v = acc[s, f, 8 : 8 + cells, :].reshape(cells // 8, 8, 192)
            left = jnp.where(col == 0, 0.0, pltpu.roll(v[:, :, 0:64], 1, 1))
            right = jnp.where(col == 7, 0.0, pltpu.roll(v[:, :, 128:192], 7, 1))
            v = (v[:, :, 64:128] + left + right).reshape(cells, 64)
            v = v + hid_ref[f, :, s * 64 : s * 64 + 64]
            alive = (plan_ref[s] >= 0) & (f < lengths_ref[s])
            parts.append(jnp.where(alive, v, 0.0))
        v = jnp.concatenate(parts, axis=1).astype(jnp.bfloat16)
        for xp in range(count):
            out_ref[xp, f] = v[xp * part : (xp + 1) * part]


def columns_kernel(got_ref, place_ref, out_ref):
    count = got_ref.shape[0]
    slots, rows, features = out_ref.shape
    x = jnp.concatenate([got_ref[i] for i in range(count)], axis=1)
    for s in range(slots):
        y = jnp.dot(
            x, place_ref[:, s * features : (s + 1) * features], preferred_element_type=jnp.float32
        )
        out_ref[s] = y.astype(jnp.bfloat16)


VMEM = pl.BlockSpec(memory_space=pltpu.VMEM)
SMEM = pl.BlockSpec(memory_space=pltpu.SMEM)


def call(kernel, scalars, arrays, outs, scratch, name, limit, flops):
    return pl.pallas_call(
        kernel,
        out_shape=outs,
        in_specs=[SMEM] * len(scalars) + [VMEM] * len(arrays),
        out_specs=jax.tree.map(lambda _: VMEM, outs),
        scratch_shapes=scratch,
        compiler_params=pltpu.CompilerParams(vmem_limit_bytes=limit * MIB),
        cost_estimate=pl.CostEstimate(flops=flops, bytes_accessed=1 << 22, transcendentals=0),
        name=name,
    )(*scalars, *arrays)


def on_device(
    latent_slabs,
    prior_latents,
    prior_features,
    lengths,
    starts,
    move_plan,
    entry_weight,
    block_weight,
    norm_gain,
    norm_shift,
):
    nx = lax.axis_size("rows")
    nr = lax.axis_size("roll")
    ny = nr // 2
    me = lax.axis_index("rows")
    roll = lax.axis_index("roll")
    slots, frames, height, widths, latents = latent_slabs.shape
    features = entry_weight.shape[1]
    share = block_weight.shape[1]
    own = nr * share
    cells = nx * height * widths

    cached = (starts > 0)[:, None, None, None, None]
    prior_lat = jnp.where(cached, prior_latents, jnp.zeros_like(prior_latents))
    lat = jnp.concatenate([prior_lat, latent_slabs], axis=1)
    lat = jnp.concatenate([lat[:, :, :, 1::-1], lat[:, :, :, :1:-1]], axis=3)
    lat = lat.reshape(slots, frames + 2, height, widths * latents)
    lats = [lat] + [
        lax.ppermute(lat, "rows", [(i, (i + d) % nx) for i in range(nx)]) for d in range(1, nx)
    ]

    feat = prior_features.reshape(slots, 2, height * widths, features)
    up = [(i, (i + 1) % nx) for i in range(nx)]
    down = [(i, (i - 1) % nx) for i in range(nx)]
    feats = [None] * nx
    feats[0] = right = left = feat
    for k in range(1, nx // 2 + 1):
        right = lax.ppermute(right, "rows", up)
        feats[k] = right
        if nx - k > k:
            left = lax.ppermute(left, "rows", down)
            feats[nx - k] = left

    wt = block_weight.T
    wts = [wt] + [
        lax.ppermute(wt, "roll", [(r, ((r // 2 + d) % ny) * 2 + r % 2) for r in range(nr)])
        for d in range(1, ny)
    ]
    half = jnp.concatenate(wts, axis=0)
    other = lax.ppermute(half, "roll", [(r, r ^ 1) for r in range(nr)])
    weights = jnp.concatenate([half, other], axis=0)

    def column(n, x):
        swap, d, i = n // (ny * share), n // share % ny, n % share
        r = (roll // 2 - d + ny) % ny * 2 + (roll % 2 + swap) % 2
        return (r * nx + x) * share + i

    select = (jnp.arange(features)[:, None] == column(jnp.arange(own), me)[None, :]).astype(jnp.bfloat16)
    entry_own = jnp.dot(entry_weight, select, preferred_element_type=jnp.float32).astype(jnp.bfloat16)

    def packed(w):
        w = w.reshape(9, 3, latents, w.shape[1])[:, ::-1].reshape(9, 3 * latents, w.shape[1])
        return jnp.pad(w, ((0, 1), (0, 64 - 3 * latents), (0, 0))).reshape(640, w.shape[2])

    line = jnp.arange(nx * slots * own)
    target = column(line % own, line // (slots * own)) + line // own % slots * features
    place = (target[:, None] == jnp.arange(slots * features)[None, :]).astype(jnp.bfloat16)

    f32, bf16 = jnp.float32, jnp.bfloat16
    me1 = me.reshape(1).astype(jnp.int32)
    act, hid = call(
        lambda *refs: entry_kernel(nx, *refs),
        [me1],
        lats + [packed(entry_weight), packed(entry_own), norm_gain[None], norm_shift[None]],
        (
            jax.ShapeDtypeStruct((slots, frames, cells, features), bf16),
            jax.ShapeDtypeStruct((frames, cells, slots * own), f32),
        ),
        [
            pltpu.VMEM((slots, frames + 2, cells + 16, widths * latents), f32),
            pltpu.VMEM((cells, 640), bf16),
            pltpu.VMEM((slots * frames * cells, features), f32),
            pltpu.VMEM((16, features), f32),
        ],
        "entry",
        30,
        5_000_000_000,
    )
    acc = call(
        new_frames_kernel,
        [],
        [act, weights],
        jax.ShapeDtypeStruct((slots, frames, cells + 16, 3 * own), f32),
        [],
        "new_frames",
        30,
        5_000_000_000,
    )
    send = call(
        lambda *refs: old_frames_kernel(nx, *refs),
        [me1, starts, lengths, move_plan],
        feats + [weights, acc, hid],
        jax.ShapeDtypeStruct((nx, frames, height * widths, slots * own), bf16),
        [
            pltpu.VMEM((slots, 2, cells, features), bf16),
            pltpu.VMEM((slots, frames, cells + 16, 3 * own), f32),
        ],
        "old_frames",
        40,
        3_000_000_000,
    )
    got = lax.all_to_all(
        send.reshape(nx, frames * height * widths, slots * own), "rows", 0, 0, tiled=True
    )
    out = call(
        columns_kernel,
        [],
        [got, place],
        jax.ShapeDtypeStruct((slots, frames * height * widths, features), bf16),
        [],
        "columns",
        20,
        400_000_000,
    )
    return out.reshape(slots, frames, height, widths, features)


def solution(mesh):
    in_specs = (
        P(("groups", "roll"), None, "rows", None, None),
        P(("groups", "roll"), None, "rows", None, None),
        P(("groups", "roll"), None, "rows", None, None),
        P(("groups", "roll")),
        P(("groups", "roll")),
        P(("groups", "roll")),
        P(),
        P(None, ("roll", "rows")),
        P(),
        P(),
    )
    out_specs = P(("groups", "roll"), None, "rows", None, None)
    return jax.shard_map(
        on_device, mesh=mesh, in_specs=in_specs, out_specs=out_specs, check_vma=False
    )
```

```python
import jax
import jax.numpy as jnp
from jax import lax
from jax.experimental import pallas as pl
from jax.experimental.pallas import tpu as pltpu
from jax.sharding import PartitionSpec as P

GROUPS = 32
EPSILON = 1e-06
MIB = 1 << 20


def nt_dot(a, b):
    return lax.dot_general(a, b, (((1,), (1,)), ((), ())), preferred_element_type=jnp.float32)


def latents_kernel(starts_ref, prior_hbm, new_hbm, out_ref, prior_ref, new_ref, sems):
    copies = [
        pltpu.make_async_copy(prior_hbm, prior_ref, sems.at[0]),
        pltpu.make_async_copy(new_hbm, new_ref, sems.at[1]),
    ]
    for copy in copies:
        copy.start()
    count, slots, total, height, lanes = out_ref.shape
    width, latents = prior_ref.shape[3:]
    spread = lax.broadcasted_iota(jnp.int32, (latents, lanes), 1) % latents
    spread = spread == lax.broadcasted_iota(jnp.int32, (latents, lanes), 0)
    spread = jnp.where(spread, 1.0, 0.0).astype(jnp.bfloat16)
    lane = lax.broadcasted_iota(jnp.int32, (total * height, width, lanes), 2) // latents
    col = lax.broadcasted_iota(jnp.int32, (total * height, width, lanes), 1)
    mine = lane == lax.rem(9 - col, 8)
    for copy in copies:
        copy.wait()
    for s in range(slots):
        prior = prior_ref[s]
        prior = jnp.where(starts_ref[s] > 0, prior, jnp.zeros_like(prior))
        v = jnp.concatenate([prior, new_ref[s]], axis=0).reshape(total * height * width, latents)
        v = jnp.dot(v, spread, preferred_element_type=jnp.float32)
        v = jnp.where(mine, v.reshape(total * height, width, lanes), 0.0)
        v = jnp.sum(v, axis=1).astype(jnp.bfloat16).reshape(total, height, lanes)
        for i in range(count):
            out_ref[i, s] = v


def column(n, x, roll, counts, share):
    nr, nx = counts
    piece, bit, owner = n // share, nr // 2, 0
    while bit:
        flip = piece // (nr // 2 // bit) % 2
        owner = owner + lax.rem(roll // bit + flip, 2) * bit
        bit = bit // 2
    return (owner * nx + x) * share + n % share


def hidden_kernel(counts, me_ref, roll_ref, *refs):
    outside, lat_ref, refs = refs[:3], refs[3], refs[4:]
    hid, own_ref, norm_ref, win, lhs, sums, wk_ref, wown_ref, *inside, sems = refs
    weight_ref, gain_ref, shift_ref = inside
    copies = [pltpu.make_async_copy(a, b, sems.at[i]) for i, (a, b) in enumerate(zip(outside, inside))]
    for copy in copies:
        copy.start()
    count, slots, total, height, lanes = lat_ref.shape
    frames = total - 2
    cells = count * height * 8
    features = gain_ref.shape[1]
    own = wown_ref.shape[1]
    latents = lanes // 8
    win[:, :, 0:8, :] = jnp.zeros((slots, total, 8, lanes), jnp.float32)
    win[:, :, cells + 8 : cells + 16, :] = jnp.zeros((slots, total, 8, lanes), jnp.float32)
    rows = slots * total * height
    lane = lax.broadcasted_iota(jnp.int32, (rows * 8, lanes), 1)
    col = lax.broadcasted_iota(jnp.int32, (rows * 8, lanes), 0) % 8
    first = jnp.where(col == 7, 16, 0)
    last = jnp.where(col == 0, 32, 48)
    keep = (lane >= first) & (lane < last)
    for xp in range(count):
        v = lat_ref[xp].astype(jnp.float32).reshape(rows, 1, lanes)
        v = jnp.broadcast_to(v, (rows, 8, lanes)).reshape(rows * 8, lanes)
        v = pltpu.roll(v, 0, 1, stride=16, stride_axis=0)
        v = jnp.where(keep, v, 0.0)
        v = v + pltpu.roll(v, 64, 1)
        start = 8 + xp * height * 8
        win[:, :, start : start + height * 8, :] = v.reshape(slots, total, height * 8, lanes)
    wk_ref[...] = jnp.zeros(wk_ref.shape, jnp.bfloat16)
    for copy in copies:
        copy.wait()
    for k in range(9):
        for w in range(3):
            at = k * 64 + (2 - w) * latents
            wk_ref[at : at + latents, :] = weight_ref[(k * 3 + w) * latents : (k * 3 + w + 1) * latents, :]
    place = lax.broadcasted_iota(jnp.int32, (features, own), 1)
    chosen = column(place, me_ref[0], roll_ref[0], counts, own // counts[0])
    chosen = chosen == lax.broadcasted_iota(jnp.int32, (features, own), 0)
    chosen = jnp.where(chosen, 1.0, 0.0).astype(jnp.bfloat16)
    wown_ref[...] = jnp.dot(wk_ref[...], chosen, preferred_element_type=jnp.float32).astype(jnp.bfloat16)
    low = lax.broadcasted_iota(jnp.int32, (cells, lanes), 1) < 64
    for s in range(slots):
        for f in range(frames):
            blk = s * frames + f
            for p in range(5):
                t, h = divmod(2 * p, 3)
                a = win[s, f + t, h * 8 : h * 8 + cells, :]
                if p < 4:
                    t, h = divmod(2 * p + 1, 3)
                    a = jnp.where(low, a, win[s, f + t, h * 8 : h * 8 + cells, :])
                lhs[:, p * lanes : (p + 1) * lanes] = a.astype(jnp.bfloat16)
            x = lhs[...]
            y = jnp.dot(x, wk_ref[...], preferred_element_type=jnp.float32)
            hid[s, f] = y
            sums[blk : blk + 1, :] = jnp.sum(y, axis=0, keepdims=True)
            sums[8 + blk : 9 + blk, :] = jnp.sum(y * y, axis=0, keepdims=True)
            own_ref[f, :, s * own : (s + 1) * own] = jnp.dot(
                x, wown_ref[...], preferred_element_type=jnp.float32
            )
    size = features // GROUPS
    gi = lax.broadcasted_iota(jnp.int32, (features, features), 0) // size
    gj = lax.broadcasted_iota(jnp.int32, (features, features), 1) // size
    same = jnp.where(gi == gj, 1.0, 0.0).astype(jnp.float32)
    means = jnp.dot(
        sums[...], same, precision=lax.Precision.HIGHEST, preferred_element_type=jnp.float32
    ) / (cells * size)
    mean = means[0:8]
    spread = means[8:16] - mean * mean
    scale = lax.rsqrt(spread + EPSILON) * gain_ref[...]
    norm_ref[0:8, :] = scale
    norm_ref[8:16, :] = shift_ref[...] - mean * scale


def active_kernel(hid_ref, norm_ref, act_ref):
    slots, frames = act_ref.shape[:2]

    def one(blk, carry):
        s, f = blk // frames, lax.rem(blk, frames)
        z = hid_ref[s, f] * norm_ref[pl.ds(blk, 1), :] + norm_ref[pl.ds(8 + blk, 1), :]
        act = (0.5 * z) * (1.0 + jnp.tanh(0.5 * z))
        act_ref[s, f] = act.astype(jnp.bfloat16)
        return carry

    lax.fori_loop(0, slots * frames, one, 0)


def taps_of(w_ref, t, h):
    k = w_ref.shape[1] // 27
    base = (t * 3 + h) * 3
    return jnp.concatenate([w_ref[:, (base + w) * k : (base + w + 1) * k] for w in range(3)], axis=0)


def gathered(halves, w_ref):
    for i, half in enumerate(halves):
        count, share, k = half.shape
        w_ref[i * count * share : (i + 1) * count * share, :] = half[...].reshape(count * share, k)


def new_frames(offsets, act_ref, w_ref, acc_ref):
    slots, frames, cells, _ = act_ref.shape
    for t in offsets:
        for h in range(3):
            taps = taps_of(w_ref, t, h)
            at = (2 - h) * 8
            for s in range(slots):
                for f in range(frames):
                    if 0 <= f + t - 2 < frames:
                        acc_ref[s, f, at : at + cells, :] += nt_dot(act_ref[s, f + t - 2], taps)


def first_offset_kernel(act_ref, mine_ref, other_ref, acc_ref, w_ref):
    gathered((mine_ref, other_ref), w_ref)
    acc_ref[...] = jnp.zeros(acc_ref.shape, jnp.float32)
    new_frames((2,), act_ref, w_ref, acc_ref)


def more_offsets_kernel(act_ref, w_ref, _, acc_ref):
    new_frames((1, 0), act_ref, w_ref, acc_ref)


def old_frames_kernel(count, me_ref, starts_ref, lengths_ref, plan_ref, *refs):
    feat_refs = refs[: count + 1]
    w_ref, own_ref, _ = refs[count + 1 : count + 4]
    out_refs = refs[count + 4 : 2 * count + 4]
    acc, feats, done = refs[2 * count + 4 :]
    slots, frames, padded_cells, _ = acc.shape
    own = w_ref.shape[0]
    cells = padded_cells - 16
    part = cells // count
    me = me_ref[0]
    toward = 1 - 2 * lax.rem(me, 2)
    for s in range(slots):
        for d in range(count):
            if d == count // 2:
                v = feat_refs[d if s < slots // 2 else count][s % (slots // 2)]
            else:
                v = feat_refs[d][s]
            xp = lax.rem(me + toward * d + count, count)
            start = pl.multiple_of(xp * part, part)
            feats[s, :, pl.ds(start, part), :] = jnp.where(starts_ref[s] > 0, v, jnp.zeros_like(v))
    for t in range(2):
        for h in range(3):
            at = (2 - h) * 8
            taps = taps_of(w_ref, t, h)
            for s in range(slots):
                for f in range(frames):
                    if f + t < 2:
                        acc[s, f, at : at + cells, :] += nt_dot(feats[s, f + t], taps)
    col = lax.broadcasted_iota(jnp.int32, (cells // 8, 8, own), 1)
    for f in range(frames):
        parts = []
        for s in range(slots):
            v = acc[s, f, 8 : 8 + cells, :].reshape(cells // 8, 8, 3 * own)
            left = jnp.where(col == 0, 0.0, pltpu.roll(v[:, :, 0:own], 1, 1))
            right = jnp.where(col == 7, 0.0, pltpu.roll(v[:, :, 2 * own :], 7, 1))
            v = (v[:, :, own : 2 * own] + left + right).reshape(cells, own)
            v = v + own_ref[f, :, s * own : (s + 1) * own]
            alive = (plan_ref[s] >= 0) & (f < lengths_ref[s])
            parts.append(jnp.where(alive, v, 0.0))
        done[f] = jnp.concatenate(parts, axis=1).astype(jnp.bfloat16)
    for d in range(count):
        start = pl.multiple_of(lax.rem(me + d, count) * part, part)
        out_refs[d][...] = done[:, pl.ds(start, part), :]


def columns_kernel(*refs):
    got, place_ref, out_ref = refs[:-2], refs[-2], refs[-1]
    slots, rows, features = out_ref.shape
    x = jnp.concatenate([g[...].reshape(rows, g.shape[2]) for g in got], axis=1)
    for s in range(slots):
        y = jnp.dot(
            x, place_ref[:, s * features : (s + 1) * features], preferred_element_type=jnp.float32
        )
        out_ref[s] = y.astype(jnp.bfloat16)


VMEM = pl.BlockSpec(memory_space=pltpu.VMEM)
HBM = pl.BlockSpec(memory_space=pl.ANY)
SMEM = pl.BlockSpec(memory_space=pltpu.SMEM)


def call(kernel, scalars, arrays, outs, scratch, limit, flops, aliases=None, outside=0):
    return pl.pallas_call(
        kernel,
        out_shape=outs,
        in_specs=[SMEM] * len(scalars) + [HBM] * outside + [VMEM] * (len(arrays) - outside),
        out_specs=jax.tree.map(lambda _: VMEM, outs),
        scratch_shapes=scratch,
        input_output_aliases=aliases or {},
        compiler_params=pltpu.CompilerParams(vmem_limit_bytes=limit * MIB),
        cost_estimate=pl.CostEstimate(flops=flops, bytes_accessed=1 << 22, transcendentals=0),
    )(*scalars, *arrays)


def on_device(
    latent_slabs,
    prior_latents,
    prior_features,
    lengths,
    starts,
    move_plan,
    entry_weight,
    block_weight,
    norm_gain,
    norm_shift,
):
    nx = lax.axis_size("rows")
    nr = lax.axis_size("roll")
    me = lax.axis_index("rows")
    roll = lax.axis_index("roll")
    slots, frames, height, widths, latents = latent_slabs.shape
    features = entry_weight.shape[1]
    share = block_weight.shape[1]
    own = nr * share
    part = height * widths
    cells = nx * part
    f32, bf16 = jnp.float32, jnp.bfloat16
    shape = jax.ShapeDtypeStruct
    me1 = me.reshape(1).astype(jnp.int32)
    turned = [[(i, (i + d) % nx) for i in range(nx)] for d in range(nx)]

    lat = call(
        latents_kernel,
        [starts],
        [prior_latents, latent_slabs],
        shape((nx, slots, frames + 2, height, widths * latents), bf16),
        [
            pltpu.VMEM(prior_latents.shape, bf16),
            pltpu.VMEM(latent_slabs.shape, bf16),
            pltpu.SemaphoreType.DMA((2,)),
        ],
        8,
        10_000_000,
        outside=2,
    )
    lat = lax.all_to_all(lat, "rows", 0, 0, tiled=True)

    feat = prior_features.reshape(slots, 2, part, features)
    one = [(i, i ^ 1) for i in range(nx)]
    two = [(i, (i - 1 + 2 * (i % 2)) % nx) for i in range(nx)]
    feats = [None] * (nx + 1)
    feats[0] = from_one = from_two = feat
    for k in range(1, nx // 2 + 1):
        to_one, to_two = from_two, from_one
        if 2 * k == nx:
            to_one, to_two = to_one[: slots // 2], to_two[slots // 2 :]
        feats[k] = from_one = lax.ppermute(to_one, "rows", one)
        from_two = lax.ppermute(to_two, "rows", two)
        feats[nx if 2 * k == nx else nx - k] = from_two

    wt = block_weight.T
    mine, bit = wt[None], nr // 2
    while bit > 1:
        came = lax.ppermute(mine, "roll", [(r, r ^ bit) for r in range(nr)])
        mine, bit = jnp.concatenate([mine, came], axis=0), bit // 2
    other = lax.ppermute(mine, "roll", [(r, r ^ 1) for r in range(nr)])

    line = jnp.arange(nx * slots * own)
    target = column(line % own, (me - line // (slots * own) + nx) % nx, roll, (nr, nx), share)
    target = target + line // own % slots * features
    place = (target[:, None] == jnp.arange(slots * features)[None, :]).astype(bf16)

    hid, hid_own, norm = call(
        lambda *refs: hidden_kernel((nr, nx), *refs),
        [me1, roll.reshape(1).astype(jnp.int32)],
        [entry_weight, norm_gain[None], norm_shift[None], lat],
        (
            shape((slots, frames, cells, features), f32),
            shape((frames, cells, slots * own), f32),
            shape((16, features), f32),
        ),
        [
            pltpu.VMEM((slots, frames + 2, cells + 16, widths * latents), f32),
            pltpu.VMEM((cells, 640), bf16),
            pltpu.VMEM((16, features), f32),
            pltpu.VMEM((640, features), bf16),
            pltpu.VMEM((640, own), bf16),
            pltpu.VMEM(entry_weight.shape, bf16),
            pltpu.VMEM((1, features), f32),
            pltpu.VMEM((1, features), f32),
            pltpu.SemaphoreType.DMA((3,)),
        ],
        24,
        5_000_000_000,
        outside=3,
    )
    act = call(active_kernel, [], [hid, norm], shape((slots, frames, cells, features), bf16), [], 16, 3_000_000_000)
    sums = shape((slots, frames, cells + 16, 3 * own), f32)
    acc, weights = call(
        first_offset_kernel, [], [act, mine, other], (sums, shape((own, wt.shape[1]), bf16)), [], 20, 3_000_000_000
    )
    acc = call(more_offsets_kernel, [], [act, weights, acc], sums, [], 20, 3_000_000_000, {2: 0})
    piece = shape((frames, part, slots * own), bf16)
    *pieces, _ = call(
        lambda *refs: old_frames_kernel(nx, *refs),
        [me1, starts, lengths, move_plan],
        feats + [weights, hid_own, acc],
        (piece,) * nx + (sums,),
        [
            pltpu.VMEM((slots, 2, cells, features), bf16),
            pltpu.VMEM((frames, cells, slots * own), bf16),
        ],
        30,
        3_000_000_000,
        {4 + nx + 3: nx},
    )
    got = [pieces[0]] + [lax.ppermute(pieces[d], "rows", turned[d]) for d in range(1, nx)]
    out = call(columns_kernel, [], [*got, place], shape((slots, frames * part, features), bf16), [], 20, 400_000_000)
    return out.reshape(slots, frames, height, widths, features)


def solution(mesh):
    in_specs = (
        P(("groups", "roll"), None, "rows", None, None),
        P(("groups", "roll"), None, "rows", None, None),
        P(("groups", "roll"), None, "rows", None, None),
        P(("groups", "roll")),
        P(("groups", "roll")),
        P(("groups", "roll")),
        P(),
        P(None, ("roll", "rows")),
        P(),
        P(),
    )
    out_specs = P(("groups", "roll"), None, "rows", None, None)

    return jax.shard_map(on_device, mesh=mesh, in_specs=in_specs, out_specs=out_specs, check_vma=False)
```

```python
import jax
import jax.numpy as jnp
from jax import lax
from jax.experimental import pallas as pl
from jax.experimental.pallas import tpu as pltpu
from jax.sharding import PartitionSpec as P

GROUPS = 32
EPSILON = 1e-06
MIB = 1 << 20


def nt_dot(a, b):
    return lax.dot_general(a, b, (((1,), (1,)), ((), ())), preferred_element_type=jnp.float32)


def latents_kernel(prior_hbm, new_hbm, out_ref, prior_ref, new_ref, sems):
    copies = [
        pltpu.make_async_copy(prior_hbm, prior_ref, sems.at[0]),
        pltpu.make_async_copy(new_hbm, new_ref, sems.at[1]),
    ]
    for copy in copies:
        copy.start()
    _, slots, total, height, lanes = out_ref.shape
    width, latents = prior_ref.shape[3:]
    spread = lax.broadcasted_iota(jnp.int32, (latents, lanes), 1) % latents
    spread = spread == lax.broadcasted_iota(jnp.int32, (latents, lanes), 0)
    spread = jnp.where(spread, 1.0, 0.0).astype(jnp.bfloat16)
    lane = lax.broadcasted_iota(jnp.int32, (total * height, width, lanes), 2) // latents
    col = lax.broadcasted_iota(jnp.int32, (total * height, width, lanes), 1)
    mine = lane == lax.rem(9 - col, 8)
    for copy in copies:
        copy.wait()
    for s in range(slots):
        v = jnp.concatenate([prior_ref[s], new_ref[s]], axis=0).reshape(total * height * width, latents)
        v = jnp.dot(v, spread, preferred_element_type=jnp.float32)
        v = jnp.where(mine, v.reshape(total * height, width, lanes), 0.0)
        out_ref[0, s] = jnp.sum(v, axis=1).astype(jnp.bfloat16).reshape(total, height, lanes)


def column(n, x, roll, counts, share):
    nr, nx = counts
    piece = n // share
    owner = piece % (nr // 2) * 2 + lax.rem(roll + piece // (nr // 2), 2)
    return (owner * nx + x) * share + n % share


def hidden_kernel(counts, me_ref, roll_ref, starts_ref, *refs):
    outside, lat_refs, refs = refs[:3], refs[3:5], refs[5:]
    hid, own_ref, norm_ref, win, lhs, sums, wk_ref, wown_ref, *inside, sems = refs
    weight_ref, gain_ref, shift_ref = inside
    copies = [pltpu.make_async_copy(a, b, sems.at[i]) for i, (a, b) in enumerate(zip(outside, inside))]
    for copy in copies:
        copy.start()
    count = counts[1]
    slots, total, height, lanes = lat_refs[0].shape[1:]
    frames = total - 2
    cells = count * height * 8
    features = gain_ref.shape[1]
    own = wown_ref.shape[1]
    latents = lanes // 8
    win[:, :, 0:8, :] = jnp.zeros((slots, total, 8, lanes), jnp.float32)
    win[:, :, cells + 8 : cells + 16, :] = jnp.zeros((slots, total, 8, lanes), jnp.float32)
    rows = total * height
    lane = lax.broadcasted_iota(jnp.int32, (rows * 8, lanes), 1)
    col = lax.broadcasted_iota(jnp.int32, (rows * 8, lanes), 0) % 8
    first = jnp.where(col == 7, 16, 0)
    last = jnp.where(col == 0, 32, 48)
    keep = (lane >= first) & (lane < last)
    frame = lax.broadcasted_iota(jnp.int32, (total, height, lanes), 0)
    for p in range(count):
        bit, flip = 1, 0
        while bit < count:
            flip, bit = flip + (p * 2 * bit // count % 2) * bit, bit * 2
        start = pl.multiple_of(8 + (me_ref[0] ^ flip) * (height * 8), 8)
        for s in range(slots):
            v = lat_refs[p * 2 // count][p % (count // 2), s].astype(jnp.float32)
            v = jnp.where((frame > 1) | (starts_ref[s] > 0), v, 0.0).reshape(rows, 1, lanes)
            v = jnp.broadcast_to(v, (rows, 8, lanes)).reshape(rows * 8, lanes)
            v = pltpu.roll(v, 0, 1, stride=16, stride_axis=0)
            v = jnp.where(keep, v, 0.0)
            v = v + pltpu.roll(v, 64, 1)
            win[s, :, pl.ds(start, height * 8), :] = v.reshape(total, height * 8, lanes)
    wk_ref[...] = jnp.zeros(wk_ref.shape, jnp.bfloat16)
    for copy in copies:
        copy.wait()
    for k in range(9):
        for w in range(3):
            at = k * 64 + (2 - w) * latents
            wk_ref[at : at + latents, :] = weight_ref[(k * 3 + w) * latents : (k * 3 + w + 1) * latents, :]
    place = lax.broadcasted_iota(jnp.int32, (features, own), 1)
    chosen = column(place, me_ref[0], roll_ref[0], counts, own // counts[0])
    chosen = chosen == lax.broadcasted_iota(jnp.int32, (features, own), 0)
    chosen = jnp.where(chosen, 1.0, 0.0).astype(jnp.bfloat16)
    wown_ref[...] = jnp.dot(wk_ref[...], chosen, preferred_element_type=jnp.float32).astype(jnp.bfloat16)
    low = lax.broadcasted_iota(jnp.int32, (cells, lanes), 1) < 64
    for s in range(slots):
        for f in range(frames):
            blk = s * frames + f
            for p in range(5):
                t, h = divmod(2 * p, 3)
                a = win[s, f + t, h * 8 : h * 8 + cells, :]
                if p < 4:
                    t, h = divmod(2 * p + 1, 3)
                    a = jnp.where(low, a, win[s, f + t, h * 8 : h * 8 + cells, :])
                lhs[:, p * lanes : (p + 1) * lanes] = a.astype(jnp.bfloat16)
            x = lhs[...]
            y = jnp.dot(x, wk_ref[...], preferred_element_type=jnp.float32)
            hid[s, f] = y
            sums[blk : blk + 1, :] = jnp.sum(y, axis=0, keepdims=True)
            sums[8 + blk : 9 + blk, :] = jnp.sum(y * y, axis=0, keepdims=True)
            own_ref[f, :, s * own : (s + 1) * own] = jnp.dot(
                x, wown_ref[...], preferred_element_type=jnp.float32
            )
    size = features // GROUPS
    gi = lax.broadcasted_iota(jnp.int32, (features, features), 0) // size
    gj = lax.broadcasted_iota(jnp.int32, (features, features), 1) // size
    same = jnp.where(gi == gj, 1.0, 0.0).astype(jnp.float32)
    means = jnp.dot(
        sums[...], same, precision=lax.Precision.HIGHEST, preferred_element_type=jnp.float32
    ) / (cells * size)
    mean = means[0:8]
    spread = means[8:16] - mean * mean
    scale = lax.rsqrt(spread + EPSILON) * gain_ref[...]
    norm_ref[0:8, :] = scale
    norm_ref[8:16, :] = shift_ref[...] - mean * scale


def active_kernel(hid_ref, norm_ref, act_ref):
    slots, frames = act_ref.shape[:2]

    def one(blk, carry):
        s, f = blk // frames, lax.rem(blk, frames)
        z = hid_ref[s, f] * norm_ref[pl.ds(blk, 1), :] + norm_ref[pl.ds(8 + blk, 1), :]
        act = (0.5 * z) * (1.0 + jnp.tanh(0.5 * z))
        act_ref[s, f] = act.astype(jnp.bfloat16)
        return carry

    lax.fori_loop(0, slots * frames, one, 0)


def taps_of(w_ref, t, h):
    k = w_ref.shape[1] // 27
    base = (t * 3 + h) * 3
    return jnp.concatenate([w_ref[:, (base + w) * k : (base + w + 1) * k] for w in range(3)], axis=0)


def gathered(halves, w_ref):
    for i, half in enumerate(halves):
        count, share, k = half.shape
        w_ref[i * count * share : (i + 1) * count * share, :] = half[...].reshape(count * share, k)


def new_frames(offsets, act_ref, w_ref, acc_ref):
    slots, frames, cells, _ = act_ref.shape
    for t in offsets:
        for h in range(3):
            taps = taps_of(w_ref, t, h)
            at = (2 - h) * 8
            for s in range(slots):
                for f in range(frames):
                    if 0 <= f + t - 2 < frames:
                        acc_ref[s, f, at : at + cells, :] += nt_dot(act_ref[s, f + t - 2], taps)


def first_offset_kernel(act_ref, mine_ref, other_ref, acc_ref, w_ref):
    gathered((mine_ref, other_ref), w_ref)
    acc_ref[...] = jnp.zeros(acc_ref.shape, jnp.float32)
    new_frames((2,), act_ref, w_ref, acc_ref)


def more_offsets_kernel(act_ref, w_ref, _, acc_ref):
    new_frames((1, 0), act_ref, w_ref, acc_ref)


def old_frames_kernel(count, me_ref, starts_ref, lengths_ref, plan_ref, *refs):
    feat_refs = refs[: count + 1]
    w_ref, own_ref, _ = refs[count + 1 : count + 4]
    out_refs = refs[count + 4 : 2 * count + 4]
    acc, feats, done = refs[2 * count + 4 :]
    slots, frames, padded_cells, _ = acc.shape
    own = w_ref.shape[0]
    cells = padded_cells - 16
    part = cells // count
    me = me_ref[0]
    toward = 1 - 2 * lax.rem(me, 2)
    for s in range(slots):
        for d in range(count):
            if d == count // 2:
                v = feat_refs[d if s < slots // 2 else count][s % (slots // 2)]
            else:
                v = feat_refs[d][s]
            xp = lax.rem(me + toward * d + count, count)
            start = pl.multiple_of(xp * part, part)
            feats[s, :, pl.ds(start, part), :] = jnp.where(starts_ref[s] > 0, v, jnp.zeros_like(v))
    for t in range(2):
        for h in range(3):
            at = (2 - h) * 8
            taps = taps_of(w_ref, t, h)
            for s in range(slots):
                for f in range(frames):
                    if f + t < 2:
                        acc[s, f, at : at + cells, :] += nt_dot(feats[s, f + t], taps)
    col = lax.broadcasted_iota(jnp.int32, (cells // 8, 8, own), 1)
    for f in range(frames):
        parts = []
        for s in range(slots):
            v = acc[s, f, 8 : 8 + cells, :].reshape(cells // 8, 8, 3 * own)
            left = jnp.where(col == 0, 0.0, pltpu.roll(v[:, :, 0:own], 1, 1))
            right = jnp.where(col == 7, 0.0, pltpu.roll(v[:, :, 2 * own :], 7, 1))
            v = (v[:, :, own : 2 * own] + left + right).reshape(cells, own)
            v = v + own_ref[f, :, s * own : (s + 1) * own]
            alive = (plan_ref[s] >= 0) & (f < lengths_ref[s])
            parts.append(jnp.where(alive, v, 0.0))
        done[f] = jnp.concatenate(parts, axis=1).astype(jnp.bfloat16)
    for d in range(count):
        start = pl.multiple_of(lax.rem(me + d, count) * part, part)
        out_refs[d][...] = done[:, pl.ds(start, part), :]


def columns_kernel(*refs):
    got, place_ref, out_ref = refs[:-2], refs[-2], refs[-1]
    slots, rows, features = out_ref.shape
    x = jnp.concatenate([g[...].reshape(rows, g.shape[2]) for g in got], axis=1)
    for s in range(slots):
        y = jnp.dot(
            x, place_ref[:, s * features : (s + 1) * features], preferred_element_type=jnp.float32
        )
        out_ref[s] = y.astype(jnp.bfloat16)


VMEM = pl.BlockSpec(memory_space=pltpu.VMEM)
HBM = pl.BlockSpec(memory_space=pltpu.HBM)
SMEM = pl.BlockSpec(memory_space=pltpu.SMEM)


def call(kernel, scalars, arrays, outs, scratch, limit, flops, aliases=None, outside=0):
    return pl.pallas_call(
        kernel,
        out_shape=outs,
        in_specs=[SMEM] * len(scalars) + [HBM] * outside + [VMEM] * (len(arrays) - outside),
        out_specs=jax.tree.map(lambda _: VMEM, outs),
        scratch_shapes=scratch,
        input_output_aliases=aliases or {},
        compiler_params=pltpu.CompilerParams(vmem_limit_bytes=limit * MIB),
        cost_estimate=pl.CostEstimate(flops=flops, bytes_accessed=1 << 22, transcendentals=0),
    )(*scalars, *arrays)


def on_device(
    latent_slabs,
    prior_latents,
    prior_features,
    lengths,
    starts,
    move_plan,
    entry_weight,
    block_weight,
    norm_gain,
    norm_shift,
):
    nx = lax.axis_size("rows")
    nr = lax.axis_size("roll")
    me = lax.axis_index("rows")
    roll = lax.axis_index("roll")
    slots, frames, height, widths, latents = latent_slabs.shape
    features = entry_weight.shape[1]
    share = block_weight.shape[1]
    own = nr * share
    part = height * widths
    cells = nx * part
    f32, bf16 = jnp.float32, jnp.bfloat16
    shape = jax.ShapeDtypeStruct
    me1 = me.reshape(1).astype(jnp.int32)
    turned = [[(i, (i + d) % nx) for i in range(nx)] for d in range(nx)]

    lat = call(
        latents_kernel,
        [],
        [prior_latents, latent_slabs],
        shape((1, slots, frames + 2, height, widths * latents), bf16),
        [
            pltpu.VMEM(prior_latents.shape, bf16),
            pltpu.VMEM(latent_slabs.shape, bf16),
            pltpu.SemaphoreType.DMA((2,)),
        ],
        8,
        10_000_000,
        outside=2,
    )
    bit = nx // 2
    while bit:
        came = lax.ppermute(lat, "rows", [(i, i ^ bit) for i in range(nx)])
        if bit > 1:
            lat = jnp.concatenate([lat, came], axis=0)
        bit = bit // 2
    lats = [lat, came]

    feat = prior_features.reshape(slots, 2, part, features)
    one = [(i, i ^ 1) for i in range(nx)]
    two = [(i, (i - 1 + 2 * (i % 2)) % nx) for i in range(nx)]
    feats = [None] * (nx + 1)
    feats[0] = from_one = from_two = feat
    for k in range(1, nx // 2 + 1):
        to_one, to_two = from_two, from_one
        if 2 * k == nx:
            to_one, to_two = to_one[: slots // 2], to_two[slots // 2 :]
        feats[k] = from_one = lax.ppermute(to_one, "rows", one)
        from_two = lax.ppermute(to_two, "rows", two)
        feats[nx if 2 * k == nx else nx - k] = from_two

    wt = block_weight.T
    same_core = [[r for r in range(nr) if r % 2 == c] for c in range(2)]
    mine = jnp.broadcast_to(wt[None], (nr // 2, *wt.shape))
    mine = lax.all_to_all(mine, "roll", 0, 0, axis_index_groups=same_core, tiled=True)
    other = lax.ppermute(mine, "roll", [(r, r ^ 1) for r in range(nr)])

    line = jnp.arange(nx * slots * own)
    target = column(line % own, (me - line // (slots * own) + nx) % nx, roll, (nr, nx), share)
    target = target + line // own % slots * features
    place = (target[:, None] == jnp.arange(slots * features)[None, :]).astype(bf16)

    hid, hid_own, norm = call(
        lambda *refs: hidden_kernel((nr, nx), *refs),
        [me1, roll.reshape(1).astype(jnp.int32), starts],
        [entry_weight, norm_gain[None], norm_shift[None], *lats],
        (
            shape((slots, frames, cells, features), f32),
            shape((frames, cells, slots * own), f32),
            shape((16, features), f32),
        ),
        [
            pltpu.VMEM((slots, frames + 2, cells + 16, widths * latents), f32),
            pltpu.VMEM((cells, 640), bf16),
            pltpu.VMEM((16, features), f32),
            pltpu.VMEM((640, features), bf16),
            pltpu.VMEM((640, own), bf16),
            pltpu.VMEM(entry_weight.shape, bf16),
            pltpu.VMEM((1, features), f32),
            pltpu.VMEM((1, features), f32),
            pltpu.SemaphoreType.DMA((3,)),
        ],
        24,
        5_000_000_000,
        outside=3,
    )
    act = call(active_kernel, [], [hid, norm], shape((slots, frames, cells, features), bf16), [], 16, 3_000_000_000)
    sums = shape((slots, frames, cells + 16, 3 * own), f32)
    acc, weights = call(
        first_offset_kernel, [], [act, mine, other], (sums, shape((own, wt.shape[1]), bf16)), [], 20, 3_000_000_000
    )
    acc = call(more_offsets_kernel, [], [act, weights, acc], sums, [], 20, 3_000_000_000, {2: 0})
    piece = shape((frames, part, slots * own), bf16)
    *pieces, _ = call(
        lambda *refs: old_frames_kernel(nx, *refs),
        [me1, starts, lengths, move_plan],
        feats + [weights, hid_own, acc],
        (piece,) * nx + (sums,),
        [
            pltpu.VMEM((slots, 2, cells, features), bf16),
            pltpu.VMEM((frames, cells, slots * own), bf16),
        ],
        30,
        3_000_000_000,
        {4 + nx + 3: nx},
    )
    got = [pieces[0]] + [lax.ppermute(pieces[d], "rows", turned[d]) for d in range(1, nx)]
    out = call(columns_kernel, [], [*got, place], shape((slots, frames * part, features), bf16), [], 20, 400_000_000)
    return out.reshape(slots, frames, height, widths, features)


def solution(mesh):
    in_specs = (
        P(("groups", "roll"), None, "rows", None, None),
        P(("groups", "roll"), None, "rows", None, None),
        P(("groups", "roll"), None, "rows", None, None),
        P(("groups", "roll")),
        P(("groups", "roll")),
        P(("groups", "roll")),
        P(),
        P(None, ("roll", "rows")),
        P(),
        P(),
    )
    out_specs = P(("groups", "roll"), None, "rows", None, None)

    return jax.shard_map(on_device, mesh=mesh, in_specs=in_specs, out_specs=out_specs, check_vma=False)
```

```python
import jax
import jax.numpy as jnp
from jax import lax
from jax.experimental import pallas as pl
from jax.experimental.pallas import tpu as pltpu
from jax.sharding import PartitionSpec as P

GROUPS = 32
EPSILON = 1e-06
MIB = 1 << 20


def nt_dot(a, b):
    return lax.dot_general(a, b, (((1,), (1,)), ((), ())), preferred_element_type=jnp.float32)


def latents_kernel(prior_hbm, new_hbm, out_ref, prior_ref, new_ref, sems):
    copies = [
        pltpu.make_async_copy(prior_hbm, prior_ref, sems.at[0]),
        pltpu.make_async_copy(new_hbm, new_ref, sems.at[1]),
    ]
    for copy in copies:
        copy.start()
    _, slots, total, height, lanes = out_ref.shape
    width, latents = prior_ref.shape[3:]
    spread = lax.broadcasted_iota(jnp.int32, (latents, lanes), 1) % latents
    spread = spread == lax.broadcasted_iota(jnp.int32, (latents, lanes), 0)
    spread = jnp.where(spread, 1.0, 0.0).astype(jnp.bfloat16)
    lane = lax.broadcasted_iota(jnp.int32, (total * height, width, lanes), 2) // latents
    col = lax.broadcasted_iota(jnp.int32, (total * height, width, lanes), 1)
    mine = lane == lax.rem(9 - col, 8)
    for copy in copies:
        copy.wait()
    for s in range(slots):
        v = jnp.concatenate([prior_ref[s], new_ref[s]], axis=0).reshape(total * height * width, latents)
        v = jnp.dot(v, spread, preferred_element_type=jnp.float32)
        v = jnp.where(mine, v.reshape(total * height, width, lanes), 0.0)
        out_ref[0, s] = jnp.sum(v, axis=1).astype(jnp.bfloat16).reshape(total, height, lanes)


def column(n, x, roll, counts, share):
    nr, nx = counts
    piece = n // share
    owner = piece % (nr // 2) * 2 + lax.rem(roll + piece // (nr // 2), 2)
    return (owner * nx + x) * share + n % share


def prepared_kernel(counts, me_ref, roll_ref, starts_ref, weight_ref, gain_ref, shift_ref, *refs):
    wk_ref, wown_ref, rows_ref, cached_ref = refs
    features, own = wk_ref.shape[1], wown_ref.shape[1]
    latents = weight_ref.shape[0] // 27
    wk_ref[...] = jnp.zeros(wk_ref.shape, jnp.bfloat16)
    for k in range(9):
        for w in range(3):
            at = k * 64 + (2 - w) * latents
            wk_ref[at : at + latents, :] = weight_ref[(k * 3 + w) * latents : (k * 3 + w + 1) * latents, :]
    place = lax.broadcasted_iota(jnp.int32, (features, own), 1)
    chosen = column(place, me_ref[0], roll_ref[0], counts, own // counts[0])
    chosen = chosen == lax.broadcasted_iota(jnp.int32, (features, own), 0)
    chosen = jnp.where(chosen, 1.0, 0.0).astype(jnp.bfloat16)
    wown_ref[...] = jnp.dot(wk_ref[...], chosen, preferred_element_type=jnp.float32).astype(jnp.bfloat16)
    rows_ref[0:1, :] = gain_ref[...]
    rows_ref[1:2, :] = shift_ref[...]
    for s in range(starts_ref.shape[0]):
        cached_ref[s : s + 1, :] = jnp.where(starts_ref[s] > 0, jnp.ones((1, 128), jnp.float32), 0.0)


def hidden_kernel(count, me_ref, *refs):
    lat_refs, refs = refs[:2], refs[2:]
    wk_ref, wown_ref, rows_ref, cached_ref, hid, own_ref, norm_ref, win, lhs, sums = refs
    slots, total, height, lanes = lat_refs[0].shape[1:]
    frames = total - 2
    cells = count * height * 8
    features = wk_ref.shape[1]
    own = wown_ref.shape[1]
    win[:, :, 0:8, :] = jnp.zeros((slots, total, 8, lanes), jnp.float32)
    win[:, :, cells + 8 : cells + 16, :] = jnp.zeros((slots, total, 8, lanes), jnp.float32)
    rows = total * height
    lane = lax.broadcasted_iota(jnp.int32, (rows * 8, lanes), 1)
    col = lax.broadcasted_iota(jnp.int32, (rows * 8, lanes), 0) % 8
    first = jnp.where(col == 7, 16, 0)
    last = jnp.where(col == 0, 32, 48)
    keep = (lane >= first) & (lane < last)
    frame = lax.broadcasted_iota(jnp.int32, (total, height, lanes), 0)
    for p in range(count):
        bit, flip = 1, 0
        while bit < count:
            flip, bit = flip + (p * 2 * bit // count % 2) * bit, bit * 2
        start = pl.multiple_of(8 + (me_ref[0] ^ flip) * (height * 8), 8)
        for s in range(slots):
            v = lat_refs[p * 2 // count][p % (count // 2), s].astype(jnp.float32)
            v = jnp.where(frame > 1, v, v * cached_ref[s : s + 1, :]).reshape(rows, 1, lanes)
            v = jnp.broadcast_to(v, (rows, 8, lanes)).reshape(rows * 8, lanes)
            v = pltpu.roll(v, 0, 1, stride=16, stride_axis=0)
            v = jnp.where(keep, v, 0.0)
            v = v + pltpu.roll(v, 64, 1)
            win[s, :, pl.ds(start, height * 8), :] = v.reshape(total, height * 8, lanes)
    low = lax.broadcasted_iota(jnp.int32, (cells, lanes), 1) < 64
    for s in range(slots):
        for f in range(frames):
            blk = s * frames + f
            for p in range(5):
                t, h = divmod(2 * p, 3)
                a = win[s, f + t, h * 8 : h * 8 + cells, :]
                if p < 4:
                    t, h = divmod(2 * p + 1, 3)
                    a = jnp.where(low, a, win[s, f + t, h * 8 : h * 8 + cells, :])
                lhs[:, p * lanes : (p + 1) * lanes] = a.astype(jnp.bfloat16)
            x = lhs[...]
            y = jnp.dot(x, wk_ref[...], preferred_element_type=jnp.float32)
            hid[s, f] = y
            sums[blk : blk + 1, :] = jnp.sum(y, axis=0, keepdims=True)
            sums[8 + blk : 9 + blk, :] = jnp.sum(y * y, axis=0, keepdims=True)
            own_ref[f, :, s * own : (s + 1) * own] = jnp.dot(
                x, wown_ref[...], preferred_element_type=jnp.float32
            )
    size = features // GROUPS
    gi = lax.broadcasted_iota(jnp.int32, (features, features), 0) // size
    gj = lax.broadcasted_iota(jnp.int32, (features, features), 1) // size
    same = jnp.where(gi == gj, 1.0, 0.0).astype(jnp.float32)
    means = jnp.dot(
        sums[...], same, precision=lax.Precision.HIGHEST, preferred_element_type=jnp.float32
    ) / (cells * size)
    mean = means[0:8]
    spread = means[8:16] - mean * mean
    scale = lax.rsqrt(spread + EPSILON) * rows_ref[0:1, :]
    norm_ref[0:8, :] = scale
    norm_ref[8:16, :] = rows_ref[1:2, :] - mean * scale


def active_kernel(hid_ref, norm_ref, act_ref):
    slots, frames = act_ref.shape[:2]

    def one(blk, carry):
        s, f = blk // frames, lax.rem(blk, frames)
        z = hid_ref[s, f] * norm_ref[pl.ds(blk, 1), :] + norm_ref[pl.ds(8 + blk, 1), :]
        act = (0.5 * z) * (1.0 + jnp.tanh(0.5 * z))
        act_ref[s, f] = act.astype(jnp.bfloat16)
        return carry

    lax.fori_loop(0, slots * frames, one, 0)


def taps_of(w_ref, t, h):
    k = w_ref.shape[1] // 27
    base = (t * 3 + h) * 3
    return jnp.concatenate([w_ref[:, (base + w) * k : (base + w + 1) * k] for w in range(3)], axis=0)


def gathered(halves, w_ref):
    for i, half in enumerate(halves):
        count, share, k = half.shape
        w_ref[i * count * share : (i + 1) * count * share, :] = half[...].reshape(count * share, k)


def new_frames(offsets, act_ref, w_ref, acc_ref):
    slots, frames, cells, _ = act_ref.shape
    for t in offsets:
        for h in range(3):
            taps = taps_of(w_ref, t, h)
            at = (2 - h) * 8
            for s in range(slots):
                for f in range(frames):
                    if 0 <= f + t - 2 < frames:
                        acc_ref[s, f, at : at + cells, :] += nt_dot(act_ref[s, f + t - 2], taps)


def first_offset_kernel(act_ref, mine_ref, other_ref, acc_ref, w_ref):
    gathered((mine_ref, other_ref), w_ref)
    acc_ref[...] = jnp.zeros(acc_ref.shape, jnp.float32)
    new_frames((2,), act_ref, w_ref, acc_ref)


def more_offsets_kernel(act_ref, w_ref, _, acc_ref):
    new_frames((1, 0), act_ref, w_ref, acc_ref)


def old_frames_kernel(count, me_ref, starts_ref, lengths_ref, plan_ref, *refs):
    feat_refs = refs[: count + 1]
    w_ref, own_ref, _ = refs[count + 1 : count + 4]
    out_refs = refs[count + 4 : 2 * count + 4]
    acc, feats, done = refs[2 * count + 4 :]
    slots, frames, padded_cells, _ = acc.shape
    own = w_ref.shape[0]
    cells = padded_cells - 16
    part = cells // count
    me = me_ref[0]
    toward = 1 - 2 * lax.rem(me, 2)
    for s in range(slots):
        for d in range(count):
            if d == count // 2:
                v = feat_refs[d if s < slots // 2 else count][s % (slots // 2)]
            else:
                v = feat_refs[d][s]
            xp = lax.rem(me + toward * d + count, count)
            start = pl.multiple_of(xp * part, part)
            feats[s, :, pl.ds(start, part), :] = jnp.where(starts_ref[s] > 0, v, jnp.zeros_like(v))
    for t in range(2):
        for h in range(3):
            at = (2 - h) * 8
            taps = taps_of(w_ref, t, h)
            for s in range(slots):
                for f in range(frames):
                    if f + t < 2:
                        acc[s, f, at : at + cells, :] += nt_dot(feats[s, f + t], taps)
    col = lax.broadcasted_iota(jnp.int32, (cells // 8, 8, own), 1)
    for f in range(frames):
        parts = []
        for s in range(slots):
            v = acc[s, f, 8 : 8 + cells, :].reshape(cells // 8, 8, 3 * own)
            left = jnp.where(col == 0, 0.0, pltpu.roll(v[:, :, 0:own], 1, 1))
            right = jnp.where(col == 7, 0.0, pltpu.roll(v[:, :, 2 * own :], 7, 1))
            v = (v[:, :, own : 2 * own] + left + right).reshape(cells, own)
            v = v + own_ref[f, :, s * own : (s + 1) * own]
            alive = (plan_ref[s] >= 0) & (f < lengths_ref[s])
            parts.append(jnp.where(alive, v, 0.0))
        done[f] = jnp.concatenate(parts, axis=1).astype(jnp.bfloat16)
    for d in range(count):
        start = pl.multiple_of(lax.rem(me + d, count) * part, part)
        out_refs[d][...] = done[:, pl.ds(start, part), :]


def columns_kernel(*refs):
    got, place_ref, out_ref = refs[:-2], refs[-2], refs[-1]
    slots, rows, features = out_ref.shape
    x = jnp.concatenate([g[...].reshape(rows, g.shape[2]) for g in got], axis=1)
    for s in range(slots):
        y = jnp.dot(
            x, place_ref[:, s * features : (s + 1) * features], preferred_element_type=jnp.float32
        )
        out_ref[s] = y.astype(jnp.bfloat16)


VMEM = pl.BlockSpec(memory_space=pltpu.VMEM)
HBM = pl.BlockSpec(memory_space=pltpu.HBM)
SMEM = pl.BlockSpec(memory_space=pltpu.SMEM)


def call(kernel, scalars, arrays, outs, scratch, limit, flops, aliases=None, outside=0):
    return pl.pallas_call(
        kernel,
        out_shape=outs,
        in_specs=[SMEM] * len(scalars) + [HBM] * outside + [VMEM] * (len(arrays) - outside),
        out_specs=jax.tree.map(lambda _: VMEM, outs),
        scratch_shapes=scratch,
        input_output_aliases=aliases or {},
        compiler_params=pltpu.CompilerParams(vmem_limit_bytes=limit * MIB),
        cost_estimate=pl.CostEstimate(flops=flops, bytes_accessed=1 << 22, transcendentals=0),
    )(*scalars, *arrays)


def on_device(
    latent_slabs,
    prior_latents,
    prior_features,
    lengths,
    starts,
    move_plan,
    entry_weight,
    block_weight,
    norm_gain,
    norm_shift,
):
    nx = lax.axis_size("rows")
    nr = lax.axis_size("roll")
    me = lax.axis_index("rows")
    roll = lax.axis_index("roll")
    slots, frames, height, widths, latents = latent_slabs.shape
    features = entry_weight.shape[1]
    share = block_weight.shape[1]
    own = nr * share
    part = height * widths
    cells = nx * part
    f32, bf16 = jnp.float32, jnp.bfloat16
    shape = jax.ShapeDtypeStruct
    me1 = me.reshape(1).astype(jnp.int32)
    turned = [[(i, (i + d) % nx) for i in range(nx)] for d in range(nx)]

    lat = call(
        latents_kernel,
        [],
        [prior_latents, latent_slabs],
        shape((1, slots, frames + 2, height, widths * latents), bf16),
        [
            pltpu.VMEM(prior_latents.shape, bf16),
            pltpu.VMEM(latent_slabs.shape, bf16),
            pltpu.SemaphoreType.DMA((2,)),
        ],
        8,
        10_000_000,
        outside=2,
    )
    bit = nx // 2
    while bit:
        came = lax.ppermute(lat, "rows", [(i, i ^ bit) for i in range(nx)])
        if bit > 1:
            lat = jnp.concatenate([lat, came], axis=0)
        bit = bit // 2
    lats = [lat, came]

    feat = prior_features.reshape(slots, 2, part, features)
    one = [(i, i ^ 1) for i in range(nx)]
    two = [(i, (i - 1 + 2 * (i % 2)) % nx) for i in range(nx)]
    feats = [None] * (nx + 1)
    feats[0] = from_one = from_two = feat
    for k in range(1, nx // 2 + 1):
        to_one, to_two = from_two, from_one
        if 2 * k == nx:
            to_one, to_two = to_one[: slots // 2], to_two[slots // 2 :]
        feats[k] = from_one = lax.ppermute(to_one, "rows", one)
        from_two = lax.ppermute(to_two, "rows", two)
        feats[nx if 2 * k == nx else nx - k] = from_two

    wt = block_weight.T
    same_core = [[r for r in range(nr) if r % 2 == c] for c in range(2)]
    mine = jnp.broadcast_to(wt[None], (nr // 2, *wt.shape))
    mine = lax.all_to_all(mine, "roll", 0, 0, axis_index_groups=same_core, tiled=True)
    other = lax.ppermute(mine, "roll", [(r, r ^ 1) for r in range(nr)])

    line = jnp.arange(nx * slots * own)
    target = column(line % own, (me - line // (slots * own) + nx) % nx, roll, (nr, nx), share)
    target = target + line // own % slots * features
    place = (target[:, None] == jnp.arange(slots * features)[None, :]).astype(bf16)

    roll1 = roll.reshape(1).astype(jnp.int32)
    prepared = call(
        lambda *refs: prepared_kernel((nr, nx), *refs),
        [me1, roll1, starts],
        [entry_weight, norm_gain[None], norm_shift[None]],
        (
            shape((640, features), bf16),
            shape((640, own), bf16),
            shape((8, features), f32),
            shape((8, widths * latents), f32),
        ),
        [],
        8,
        100_000_000,
    )
    hid, hid_own, norm = call(
        lambda *refs: hidden_kernel(nx, *refs),
        [me1],
        [*lats, *prepared],
        (
            shape((slots, frames, cells, features), f32),
            shape((frames, cells, slots * own), f32),
            shape((16, features), f32),
        ),
        [
            pltpu.VMEM((slots, frames + 2, cells + 16, widths * latents), f32),
            pltpu.VMEM((cells, 640), bf16),
            pltpu.VMEM((16, features), f32),
        ],
        24,
        5_000_000_000,
    )
    act = call(active_kernel, [], [hid, norm], shape((slots, frames, cells, features), bf16), [], 16, 3_000_000_000)
    sums = shape((slots, frames, cells + 16, 3 * own), f32)
    acc, weights = call(
        first_offset_kernel, [], [act, mine, other], (sums, shape((own, wt.shape[1]), bf16)), [], 20, 3_000_000_000
    )
    acc = call(more_offsets_kernel, [], [act, weights, acc], sums, [], 20, 3_000_000_000, {2: 0})
    piece = shape((frames, part, slots * own), bf16)
    *pieces, _ = call(
        lambda *refs: old_frames_kernel(nx, *refs),
        [me1, starts, lengths, move_plan],
        feats + [weights, hid_own, acc],
        (piece,) * nx + (sums,),
        [
            pltpu.VMEM((slots, 2, cells, features), bf16),
            pltpu.VMEM((frames, cells, slots * own), bf16),
        ],
        30,
        3_000_000_000,
        {4 + nx + 3: nx},
    )
    got = [pieces[0]] + [lax.ppermute(pieces[d], "rows", turned[d]) for d in range(1, nx)]
    out = call(columns_kernel, [], [*got, place], shape((slots, frames * part, features), bf16), [], 20, 400_000_000)
    return out.reshape(slots, frames, height, widths, features)


def solution(mesh):
    in_specs = (
        P(("groups", "roll"), None, "rows", None, None),
        P(("groups", "roll"), None, "rows", None, None),
        P(("groups", "roll"), None, "rows", None, None),
        P(("groups", "roll")),
        P(("groups", "roll")),
        P(("groups", "roll")),
        P(),
        P(None, ("roll", "rows")),
        P(),
        P(),
    )
    out_specs = P(("groups", "roll"), None, "rows", None, None)

    return jax.shard_map(on_device, mesh=mesh, in_specs=in_specs, out_specs=out_specs, check_vma=False)
```

```python
import jax
import jax.numpy as jnp
from jax import lax
from jax.experimental import pallas as pl
from jax.experimental.pallas import tpu as pltpu
from jax.sharding import PartitionSpec as P

GROUPS = 32
EPSILON = 1e-06
MIB = 1 << 20


def nt_dot(a, b):
    return lax.dot_general(a, b, (((1,), (1,)), ((), ())), preferred_element_type=jnp.float32)


def latents_kernel(prior_hbm, new_hbm, out_ref, prior_ref, new_ref, sems):
    copies = [
        pltpu.make_async_copy(prior_hbm, prior_ref, sems.at[0]),
        pltpu.make_async_copy(new_hbm, new_ref, sems.at[1]),
    ]
    for copy in copies:
        copy.start()
    _, slots, total, height, lanes = out_ref.shape
    width, latents = prior_ref.shape[3:]
    spread = lax.broadcasted_iota(jnp.int32, (latents, lanes), 1) % latents
    spread = spread == lax.broadcasted_iota(jnp.int32, (latents, lanes), 0)
    spread = jnp.where(spread, 1.0, 0.0).astype(jnp.bfloat16)
    lane = lax.broadcasted_iota(jnp.int32, (total * height, width, lanes), 2) // latents
    col = lax.broadcasted_iota(jnp.int32, (total * height, width, lanes), 1)
    mine = lane == lax.rem(9 - col, 8)
    for copy in copies:
        copy.wait()
    for s in range(slots):
        v = jnp.concatenate([prior_ref[s], new_ref[s]], axis=0).reshape(total * height * width, latents)
        v = jnp.dot(v, spread, preferred_element_type=jnp.float32)
        v = jnp.where(mine, v.reshape(total * height, width, lanes), 0.0)
        out_ref[0, s] = jnp.sum(v, axis=1).astype(jnp.bfloat16).reshape(total, height, lanes)


def column(n, x, roll, counts, share):
    nr, nx = counts
    piece = n // share
    owner = piece % (nr // 2) * 2 + lax.rem(roll + piece // (nr // 2), 2)
    return (owner * nx + x) * share + n % share


def prepared_kernel(counts, me_ref, roll_ref, starts_ref, weight_ref, gain_ref, shift_ref, *refs):
    wk_ref, wown_ref, rows_ref, cached_ref = refs
    features, own = wk_ref.shape[1], wown_ref.shape[1]
    latents = weight_ref.shape[0] // 27
    wk_ref[...] = jnp.zeros(wk_ref.shape, jnp.bfloat16)
    for k in range(9):
        for w in range(3):
            at = k * 64 + (2 - w) * latents
            wk_ref[at : at + latents, :] = weight_ref[(k * 3 + w) * latents : (k * 3 + w + 1) * latents, :]
    place = lax.broadcasted_iota(jnp.int32, (features, own), 1)
    chosen = column(place, me_ref[0], roll_ref[0], counts, own // counts[0])
    chosen = chosen == lax.broadcasted_iota(jnp.int32, (features, own), 0)
    chosen = jnp.where(chosen, 1.0, 0.0).astype(jnp.bfloat16)
    wown_ref[...] = jnp.dot(wk_ref[...], chosen, preferred_element_type=jnp.float32).astype(jnp.bfloat16)
    rows_ref[0:1, :] = gain_ref[...]
    rows_ref[1:2, :] = shift_ref[...]
    for s in range(starts_ref.shape[0]):
        cached_ref[s : s + 1, :] = jnp.where(starts_ref[s] > 0, jnp.ones((1, 128), jnp.float32), 0.0)


def hidden_kernel(count, me_ref, *refs):
    lat_refs, refs = refs[:2], refs[2:]
    wk_ref, wown_ref, rows_ref, cached_ref, hid, own_ref, norm_ref, win, lhs, sums = refs
    slots, total, height, lanes = lat_refs[0].shape[1:]
    frames = total - 2
    cells = count * height * 8
    features = wk_ref.shape[1]
    own = wown_ref.shape[1]
    win[:, :, 0:8, :] = jnp.zeros((slots, total, 8, lanes), jnp.float32)
    win[:, :, cells + 8 : cells + 16, :] = jnp.zeros((slots, total, 8, lanes), jnp.float32)
    rows = total * height
    lane = lax.broadcasted_iota(jnp.int32, (rows * 8, lanes), 1)
    col = lax.broadcasted_iota(jnp.int32, (rows * 8, lanes), 0) % 8
    first = jnp.where(col == 7, 16, 0)
    last = jnp.where(col == 0, 32, 48)
    keep = (lane >= first) & (lane < last)
    frame = lax.broadcasted_iota(jnp.int32, (total, height, lanes), 0)
    for p in range(count):
        bit, flip = 1, 0
        while bit < count:
            flip, bit = flip + (p * 2 * bit // count % 2) * bit, bit * 2
        start = pl.multiple_of(8 + (me_ref[0] ^ flip) * (height * 8), 8)
        for s in range(slots):
            v = lat_refs[p * 2 // count][p % (count // 2), s].astype(jnp.float32)
            v = jnp.where(frame > 1, v, v * cached_ref[s : s + 1, :]).reshape(rows, 1, lanes)
            v = jnp.broadcast_to(v, (rows, 8, lanes)).reshape(rows * 8, lanes)
            v = pltpu.roll(v, 0, 1, stride=16, stride_axis=0)
            v = jnp.where(keep, v, 0.0)
            v = v + pltpu.roll(v, 64, 1)
            win[s, :, pl.ds(start, height * 8), :] = v.reshape(total, height * 8, lanes)
    low = lax.broadcasted_iota(jnp.int32, (cells, lanes), 1) < 64
    for s in range(slots):
        for f in range(frames):
            blk = s * frames + f
            for p in range(5):
                t, h = divmod(2 * p, 3)
                a = win[s, f + t, h * 8 : h * 8 + cells, :]
                if p < 4:
                    t, h = divmod(2 * p + 1, 3)
                    a = jnp.where(low, a, win[s, f + t, h * 8 : h * 8 + cells, :])
                lhs[:, p * lanes : (p + 1) * lanes] = a.astype(jnp.bfloat16)
            x = lhs[...]
            y = jnp.dot(x, wk_ref[...], preferred_element_type=jnp.float32)
            hid[s, f] = y
            sums[blk : blk + 1, :] = jnp.sum(y, axis=0, keepdims=True)
            sums[8 + blk : 9 + blk, :] = jnp.sum(y * y, axis=0, keepdims=True)
            own_ref[f, :, s * own : (s + 1) * own] = jnp.dot(
                x, wown_ref[...], preferred_element_type=jnp.float32
            )
    size = features // GROUPS
    gi = lax.broadcasted_iota(jnp.int32, (features, features), 0) // size
    gj = lax.broadcasted_iota(jnp.int32, (features, features), 1) // size
    same = jnp.where(gi == gj, 1.0, 0.0).astype(jnp.float32)
    means = jnp.dot(
        sums[...], same, precision=lax.Precision.HIGHEST, preferred_element_type=jnp.float32
    ) / (cells * size)
    mean = means[0:8]
    spread = means[8:16] - mean * mean
    scale = lax.rsqrt(spread + EPSILON) * rows_ref[0:1, :]
    norm_ref[0:8, :] = scale
    norm_ref[8:16, :] = rows_ref[1:2, :] - mean * scale


def active_kernel(hid_ref, norm_ref, act_ref):
    slots, frames = act_ref.shape[:2]

    def one(blk, carry):
        s, f = blk // frames, lax.rem(blk, frames)
        z = hid_ref[s, f] * norm_ref[pl.ds(blk, 1), :] + norm_ref[pl.ds(8 + blk, 1), :]
        act = (0.5 * z) * (1.0 + jnp.tanh(0.5 * z))
        act_ref[s, f] = act.astype(jnp.bfloat16)
        return carry

    lax.fori_loop(0, slots * frames, one, 0)


def taps_of(w_ref, t, h):
    k = w_ref.shape[1] // 27
    base = (t * 3 + h) * 3
    return jnp.concatenate([w_ref[:, (base + w) * k : (base + w + 1) * k] for w in range(3)], axis=0)


def gathered(halves, w_ref):
    for i, half in enumerate(halves):
        count, share, k = half.shape
        w_ref[i * count * share : (i + 1) * count * share, :] = half[...].reshape(count * share, k)


def new_frames(offsets, act_ref, w_ref, acc_ref):
    slots, frames, cells, _ = act_ref.shape
    for t in offsets:
        for h in range(3):
            taps = taps_of(w_ref, t, h)
            at = (2 - h) * 8
            for s in range(slots):
                for f in range(frames):
                    if 0 <= f + t - 2 < frames:
                        acc_ref[s, f, at : at + cells, :] += nt_dot(act_ref[s, f + t - 2], taps)


def first_offset_kernel(act_ref, mine_ref, other_ref, acc_ref, w_ref):
    gathered((mine_ref, other_ref), w_ref)
    acc_ref[...] = jnp.zeros(acc_ref.shape, jnp.float32)
    new_frames((2,), act_ref, w_ref, acc_ref)


def more_offsets_kernel(act_ref, w_ref, _, acc_ref):
    new_frames((1, 0), act_ref, w_ref, acc_ref)


def near_features_kernel(count, me_ref, starts_ref, *refs):
    feat_refs = refs[: count - 1]
    w_ref, _, acc, feats = refs[count - 1 :]
    slots, frames, padded_cells, _ = acc.shape
    cells = padded_cells - 16
    part = cells // count
    me = me_ref[0]
    toward = 1 - 2 * lax.rem(me, 2)
    for s in range(slots):
        for d in range(count):
            xp = lax.rem(me + toward * d + count, count)
            start = pl.multiple_of(xp * part, part)
            if d == count // 2:
                v = jnp.zeros((2, part, feats.shape[3]), feats.dtype)
            else:
                v = feat_refs[d - (d > count // 2)][s]
                v = jnp.where(starts_ref[s] > 0, v, jnp.zeros_like(v))
            feats[s, :, pl.ds(start, part), :] = v
    for t in range(2):
        for h in range(3):
            at = (2 - h) * 8
            taps = taps_of(w_ref, t, h)
            for s in range(slots):
                for f in range(frames):
                    if f + t < 2:
                        acc[s, f, at : at + cells, :] += nt_dot(feats[s, f + t], taps)


def far_features_kernel(count, me_ref, starts_ref, lengths_ref, plan_ref, *refs):
    far_refs, (w_ref, own_ref, _) = refs[:2], refs[2:5]
    out_refs = refs[5 : count + 5]
    acc, done = refs[count + 5 :]
    slots, frames, padded_cells, _ = acc.shape
    own = w_ref.shape[0]
    cells = padded_cells - 16
    part = cells // count
    me = me_ref[0]
    far = []
    for s in range(slots):
        v = far_refs[s // (slots // 2)][s % (slots // 2)]
        far.append(jnp.where(starts_ref[s] > 0, v, jnp.zeros_like(v)))
    for t in range(2):
        for h in range(3):
            start = lax.rem(me + count // 2, count) * part + (2 - h) * 8
            rows = pl.ds(pl.multiple_of(start, 8), part)
            taps = taps_of(w_ref, t, h)
            for s in range(slots):
                for f in range(frames):
                    if f + t < 2:
                        acc[s, f, rows, :] += nt_dot(far[s][f + t], taps)
    col = lax.broadcasted_iota(jnp.int32, (cells // 8, 8, own), 1)
    for f in range(frames):
        parts = []
        for s in range(slots):
            v = acc[s, f, 8 : 8 + cells, :].reshape(cells // 8, 8, 3 * own)
            left = jnp.where(col == 0, 0.0, pltpu.roll(v[:, :, 0:own], 1, 1))
            right = jnp.where(col == 7, 0.0, pltpu.roll(v[:, :, 2 * own :], 7, 1))
            v = (v[:, :, own : 2 * own] + left + right).reshape(cells, own)
            v = v + own_ref[f, :, s * own : (s + 1) * own]
            alive = (plan_ref[s] >= 0) & (f < lengths_ref[s])
            parts.append(jnp.where(alive, v, 0.0))
        done[f] = jnp.concatenate(parts, axis=1).astype(jnp.bfloat16)
    for d in range(count):
        start = pl.multiple_of(lax.rem(me + d, count) * part, part)
        out_refs[d][...] = done[:, pl.ds(start, part), :]


def columns_kernel(*refs):
    got, place_ref, out_ref = refs[:-2], refs[-2], refs[-1]
    slots, rows, features = out_ref.shape
    x = jnp.concatenate([g[...].reshape(rows, g.shape[2]) for g in got], axis=1)
    for s in range(slots):
        y = jnp.dot(
            x, place_ref[:, s * features : (s + 1) * features], preferred_element_type=jnp.float32
        )
        out_ref[s] = y.astype(jnp.bfloat16)


VMEM = pl.BlockSpec(memory_space=pltpu.VMEM)
HBM = pl.BlockSpec(memory_space=pltpu.HBM)
SMEM = pl.BlockSpec(memory_space=pltpu.SMEM)


def call(kernel, scalars, arrays, outs, scratch, limit, flops, aliases=None, outside=0):
    return pl.pallas_call(
        kernel,
        out_shape=outs,
        in_specs=[SMEM] * len(scalars) + [HBM] * outside + [VMEM] * (len(arrays) - outside),
        out_specs=jax.tree.map(lambda _: VMEM, outs),
        scratch_shapes=scratch,
        input_output_aliases=aliases or {},
        compiler_params=pltpu.CompilerParams(vmem_limit_bytes=limit * MIB),
        cost_estimate=pl.CostEstimate(flops=flops, bytes_accessed=1 << 22, transcendentals=0),
    )(*scalars, *arrays)


def on_device(
    latent_slabs,
    prior_latents,
    prior_features,
    lengths,
    starts,
    move_plan,
    entry_weight,
    block_weight,
    norm_gain,
    norm_shift,
):
    nx = lax.axis_size("rows")
    nr = lax.axis_size("roll")
    me = lax.axis_index("rows")
    roll = lax.axis_index("roll")
    slots, frames, height, widths, latents = latent_slabs.shape
    features = entry_weight.shape[1]
    share = block_weight.shape[1]
    own = nr * share
    part = height * widths
    cells = nx * part
    f32, bf16 = jnp.float32, jnp.bfloat16
    shape = jax.ShapeDtypeStruct
    me1 = me.reshape(1).astype(jnp.int32)
    turned = [[(i, (i + d) % nx) for i in range(nx)] for d in range(nx)]

    lat = call(
        latents_kernel,
        [],
        [prior_latents, latent_slabs],
        shape((1, slots, frames + 2, height, widths * latents), bf16),
        [
            pltpu.VMEM(prior_latents.shape, bf16),
            pltpu.VMEM(latent_slabs.shape, bf16),
            pltpu.SemaphoreType.DMA((2,)),
        ],
        8,
        10_000_000,
        outside=2,
    )
    bit = nx // 2
    while bit:
        came = lax.ppermute(lat, "rows", [(i, i ^ bit) for i in range(nx)])
        if bit > 1:
            lat = jnp.concatenate([lat, came], axis=0)
        bit = bit // 2
    lats = [lat, came]

    feat = prior_features.reshape(slots, 2, part, features)
    one = [(i, i ^ 1) for i in range(nx)]
    two = [(i, (i - 1 + 2 * (i % 2)) % nx) for i in range(nx)]
    feats = [None] * (nx + 1)
    feats[0] = from_one = from_two = feat
    for k in range(1, nx // 2 + 1):
        to_one, to_two = from_two, from_one
        if 2 * k == nx:
            to_one, to_two = to_one[: slots // 2], to_two[slots // 2 :]
        feats[k] = from_one = lax.ppermute(to_one, "rows", one)
        from_two = lax.ppermute(to_two, "rows", two)
        feats[nx if 2 * k == nx else nx - k] = from_two

    wt = block_weight.T
    same_core = [[r for r in range(nr) if r % 2 == c] for c in range(2)]
    mine = jnp.broadcast_to(wt[None], (nr // 2, *wt.shape))
    mine = lax.all_to_all(mine, "roll", 0, 0, axis_index_groups=same_core, tiled=True)
    other = lax.ppermute(mine, "roll", [(r, r ^ 1) for r in range(nr)])

    line = jnp.arange(nx * slots * own)
    target = column(line % own, (me - line // (slots * own) + nx) % nx, roll, (nr, nx), share)
    target = target + line // own % slots * features
    place = (target[:, None] == jnp.arange(slots * features)[None, :]).astype(bf16)

    roll1 = roll.reshape(1).astype(jnp.int32)
    prepared = call(
        lambda *refs: prepared_kernel((nr, nx), *refs),
        [me1, roll1, starts],
        [entry_weight, norm_gain[None], norm_shift[None]],
        (
            shape((640, features), bf16),
            shape((640, own), bf16),
            shape((8, features), f32),
            shape((8, widths * latents), f32),
        ),
        [],
        8,
        100_000_000,
    )
    hid, hid_own, norm = call(
        lambda *refs: hidden_kernel(nx, *refs),
        [me1],
        [*lats, *prepared],
        (
            shape((slots, frames, cells, features), f32),
            shape((frames, cells, slots * own), f32),
            shape((16, features), f32),
        ),
        [
            pltpu.VMEM((slots, frames + 2, cells + 16, widths * latents), f32),
            pltpu.VMEM((cells, 640), bf16),
            pltpu.VMEM((16, features), f32),
        ],
        24,
        5_000_000_000,
    )
    act = call(active_kernel, [], [hid, norm], shape((slots, frames, cells, features), bf16), [], 16, 3_000_000_000)
    sums = shape((slots, frames, cells + 16, 3 * own), f32)
    acc, weights = call(
        first_offset_kernel, [], [act, mine, other], (sums, shape((own, wt.shape[1]), bf16)), [], 20, 3_000_000_000
    )
    acc = call(more_offsets_kernel, [], [act, weights, acc], sums, [], 20, 3_000_000_000, {2: 0})
    near = [feats[d] for d in range(nx) if d != nx // 2]
    acc = call(
        lambda *refs: near_features_kernel(nx, *refs),
        [me1, starts],
        near + [weights, acc],
        sums,
        [pltpu.VMEM((slots, 2, cells, features), bf16)],
        30,
        3_000_000_000,
        {2 + nx: 0},
    )
    piece = shape((frames, part, slots * own), bf16)
    *pieces, _ = call(
        lambda *refs: far_features_kernel(nx, *refs),
        [me1, starts, lengths, move_plan],
        [feats[nx // 2], feats[nx], weights, hid_own, acc],
        (piece,) * nx + (sums,),
        [pltpu.VMEM((frames, cells, slots * own), bf16)],
        20,
        1_000_000_000,
        {8: nx},
    )
    got = [pieces[0]] + [lax.ppermute(pieces[d], "rows", turned[d]) for d in range(1, nx)]
    out = call(columns_kernel, [], [*got, place], shape((slots, frames * part, features), bf16), [], 20, 400_000_000)
    return out.reshape(slots, frames, height, widths, features)


def solution(mesh):
    in_specs = (
        P(("groups", "roll"), None, "rows", None, None),
        P(("groups", "roll"), None, "rows", None, None),
        P(("groups", "roll"), None, "rows", None, None),
        P(("groups", "roll")),
        P(("groups", "roll")),
        P(("groups", "roll")),
        P(),
        P(None, ("roll", "rows")),
        P(),
        P(),
    )
    out_specs = P(("groups", "roll"), None, "rows", None, None)

    return jax.shard_map(on_device, mesh=mesh, in_specs=in_specs, out_specs=out_specs, check_vma=False)
```
